128 devices in a mesh: dev: 8 (over z_hi, y), ma: 16 (over z_lo, x, core).
Axes of the slice: x: 4, y: 4, z: 4 (z_hi: 2, z_lo: 2; z = z_hi * 2 + z_lo), core: 2. Of those that a mesh axis runs over, the one named last changes fastest.
Arguments:
- joined_weight: bfloat16 [8, 4096, 6144], P(None, 'dev', 'ma'), may hold values from -6 to 6
- norm_gain: float32 [8, 4096], P(None, 'ma'), may hold values from 0.5 to 1.5
- rotary_order: int32 [128], replicated, may hold values from 0 to 127, each once
Outputs:
- query_weight: bfloat16 [8, 4096, 4096], P(None, 'dev', 'ma')
- key_weight: bfloat16 [8, 1024, 4096], P(None, 'dev', 'ma')
- value_weight: bfloat16 [8, 1024, 4096], P(None, 'dev', 'ma')
- row_peak: float32 [8, 6144], P(None, 'dev')
The draws below stay inside these ranges and needn't reach their ends.
Inputs may be any that keep to these rules, and one draw needn't show every extreme that they name: rotary_order holds every number of 0 to 127 exactly once.
All inputs are finite; a program needn't handle non-finite values.
Results may differ from the reference program's by a relative error of at most 0.0055.
Values may be sent and summed in bfloat16 or wider, within the bound.
No kernel may reach another device: no remote copies, remote signals or barrier semaphores. Data moves between devices by JAX's collectives and lax.ppermute only.
A program may use at most 128 MiB of HBM per device.

```python
import jax
import jax.numpy as jnp

D = 4096
HEADS = 32
KV_HEADS = 8
HEAD_DIM = 128
LAYERS = 8
GROUP = 4
QKV_COLS = 6144


def shard_levels(stream_key, shape, pieces, low, top_value):
    def one(position, parts):
        steps = jax.random.uniform(jax.random.fold_in(jax.random.fold_in(stream_key, 6), position), (parts,), jnp.float32, low / len(pieces), top_value / len(pieces))
        return jnp.repeat(jnp.exp(steps), shape[position] // parts).reshape((-1,) + (1,) * (len(shape) - position - 1))

    level = one(*pieces[0])
    for cut in pieces[1:]:
        level = level * one(*cut)
    return level


def bell_draw(stream_key, extent, width, reach, cuts=(), kind=jnp.bfloat16):
    drawn = jax.random.normal(stream_key, extent, jnp.float32) * width
    if len(cuts) > 0:
        drawn = shard_levels(stream_key, extent, cuts, -0.22, 0.18) * drawn
    return jnp.clip(drawn, min=-reach, max=reach).astype(kind)


def setup_inputs(seed: int = 0) -> dict:
    keys = jax.random.split(jax.random.key(seed), 4)
    return {
        "joined_weight": bell_draw(keys[0], (LAYERS, D, QKV_COLS), 1.0, 6.0, ((1, 8), (2, 16))),
        "norm_gain": jnp.clip(1.0 + 0.1 * jax.random.normal(keys[1], (LAYERS, D), jnp.float32), 0.5, 1.5),
        "rotary_order": jax.random.permutation(keys[2], HEAD_DIM).astype(jnp.int32),
    }


def arrange_whole(stored_layer):
    head_total = HEADS + 2 * KV_HEADS
    split = stored_layer.reshape(1, D, HEAD_DIM, head_total)
    slots_query = split[..., :HEADS].reshape(1, D, HEAD_DIM, KV_HEADS, GROUP)
    slots_key = split[..., HEADS:HEADS + KV_HEADS][..., None]
    slots_value = split[..., HEADS + KV_HEADS:][..., None]
    grouped = jnp.concatenate([slots_query, slots_key, slots_value], axis=4)
    return jnp.transpose(grouped, (0, 3, 4, 2, 1))


def finish_tiles(canonical, gain_rows, rotary_order):
    layer_count = canonical.shape[0]
    column_count = canonical.shape[4]
    turned = jnp.take(canonical[:, :, :GROUP + 1], rotary_order, axis=3)
    complete = jnp.concatenate([turned, canonical[:, :, GROUP + 1:]], axis=2)
    scaled = (complete.astype(jnp.float32) * gain_rows[:, None, None, None, :]).astype(jnp.bfloat16)
    query_rows = scaled[:, :, :GROUP].reshape(layer_count, -1, column_count)
    key_rows = scaled[:, :, GROUP].reshape(layer_count, -1, column_count)
    value_rows = scaled[:, :, GROUP + 1].reshape(layer_count, -1, column_count)
    local_peak = jnp.max(jnp.abs(scaled.astype(jnp.float32)), axis=4).reshape(layer_count, -1)
    return query_rows, key_rows, value_rows, local_peak


def reference(joined_weight, norm_gain, rotary_order):
    collected = []
    for layer_index in range(LAYERS):
        canonical = arrange_whole(joined_weight[layer_index])
        gain_rows = norm_gain[layer_index:layer_index + 1]
        collected.append(finish_tiles(canonical, gain_rows, rotary_order))
    query_weight = jnp.concatenate([item[0] for item in collected], axis=0)
    key_weight = jnp.concatenate([item[1] for item in collected], axis=0)
    value_weight = jnp.concatenate([item[2] for item in collected], axis=0)
    row_peak = jnp.concatenate([item[3] for item in collected], axis=0)
    return query_weight, key_weight, value_weight, row_peak
```

```python
import jax
import jax.numpy as jnp
import numpy as np
from jax import lax
from jax.experimental import pallas as pl
from jax.experimental.pallas import tpu as pltpu
from jax.sharding import PartitionSpec as P

HEADS = 32
KV_HEADS = 8
GROUP = 4
SLOTS = GROUP + 2
HEAD_TOTAL = HEADS + 2 * KV_HEADS
BOTH = ("dev", "ma")

PAIRED = [
    [(ap * 4 + y) * 16 + (ap ^ key) * 8 + low for ap in range(2) for y in range(4)]
    for key in range(2)
    for low in range(8)
]


def picker(piece):
    columns = piece * HEAD_TOTAL
    pick = np.zeros((columns, columns), np.float32)
    for g in range(KV_HEADS):
        for s in range(SLOTS):
            head = g * GROUP + s if s < GROUP else HEADS + (s - GROUP) * KV_HEADS + g
            for d in range(piece):
                pick[(g * SLOTS + s) * piece + d, d * HEAD_TOTAL + head] = 1.0
    return jnp.asarray(pick, jnp.bfloat16)


def prepare_body(pick_ref, stored_ref, out_ref):
    rows = out_ref.shape[3]
    width = out_ref.shape[4]
    turned = lax.dot_general(
        pick_ref[...], stored_ref[0], (((1,), (1,)), ((), ())), preferred_element_type=jnp.float32
    ).astype(jnp.bfloat16)
    for g in range(KV_HEADS):
        for half in range(2):
            out_ref[g, half, 0] = turned[g * rows : (g + 1) * rows, half * width : (half + 1) * width]


def prepare(stored, piece):
    layers, features, columns = stored.shape
    rows = SLOTS * piece
    width = features // 2
    return pl.pallas_call(
        prepare_body,
        grid=(layers,),
        in_specs=[
            pl.BlockSpec((columns, columns), lambda l: (0, 0)),
            pl.BlockSpec((1, features, columns), lambda l: (l, 0, 0)),
        ],
        out_specs=pl.BlockSpec((KV_HEADS, 2, 1, rows, width), lambda l: (0, 0, l, 0, 0)),
        out_shape=jax.ShapeDtypeStruct((KV_HEADS, 2, layers, rows, width), jnp.bfloat16),
        name="prepare",
    )(picker(piece), stored)


def finish_body(turn_ref, gain_ref, moved_ref, query_ref, key_ref, value_ref, peak_ref):
    pieces = moved_ref.shape[0]
    width = moved_ref.shape[3]
    piece = moved_ref.shape[2] // SLOTS
    dim = pieces * piece
    gain = gain_ref[0]
    for s in range(SLOTS):
        rows = moved_ref[:, 0, s * piece : (s + 1) * piece, :].reshape(dim, width)
        turned = jnp.dot(turn_ref[s // (SLOTS - 1)], rows, preferred_element_type=jnp.float32)
        scaled = (turned * gain).astype(jnp.bfloat16)
        if s < GROUP:
            query_ref[0, s * dim : (s + 1) * dim, :] = scaled
        elif s == GROUP:
            key_ref[0] = scaled
        else:
            value_ref[0] = scaled
        size = jnp.abs(scaled.astype(jnp.float32))
        size = jnp.maximum(size[:, :128], size[:, 128:])
        peak_ref[0, :, s * dim : (s + 1) * dim] = jnp.max(size.T, axis=0, keepdims=True)


def finish(moved, turn, gain, dim):
    pieces, layers, rows, width = moved.shape
    return pl.pallas_call(
        finish_body,
        grid=(layers,),
        in_specs=[
            pl.BlockSpec((2, dim, dim), lambda l: (0, 0, 0)),
            pl.BlockSpec((1, 1, width), lambda l: (l, 0, 0)),
            pl.BlockSpec((pieces, 1, rows, width), lambda l: (0, l, 0, 0)),
        ],
        out_specs=[
            pl.BlockSpec((1, GROUP * dim, width), lambda l: (l, 0, 0)),
            pl.BlockSpec((1, dim, width), lambda l: (l, 0, 0)),
            pl.BlockSpec((1, dim, width), lambda l: (l, 0, 0)),
            pl.BlockSpec((1, 1, SLOTS * dim), lambda l: (l, 0, 0)),
        ],
        out_shape=[
            jax.ShapeDtypeStruct((layers, GROUP * dim, width), jnp.bfloat16),
            jax.ShapeDtypeStruct((layers, dim, width), jnp.bfloat16),
            jax.ShapeDtypeStruct((layers, dim, width), jnp.bfloat16),
            jax.ShapeDtypeStruct((layers, 1, SLOTS * dim), jnp.float32),
        ],
        name="finish",
    )(turn, gain[:, None, :], moved)


def turning(rotary_order):
    dim = rotary_order.shape[0]
    flip = (lax.axis_index("ma") // 8) ^ (lax.axis_index("dev") // 4)
    holds = jnp.arange(dim, dtype=jnp.int32) ^ (flip * (dim // 2))
    orders = jnp.stack([rotary_order, jnp.arange(dim, dtype=jnp.int32)])
    return (orders[:, :, None] == holds[None, None, :]).astype(jnp.bfloat16)


def shards(joined_weight, norm_gain, rotary_order):
    layers, features, columns = joined_weight.shape
    piece = columns // HEAD_TOTAL
    dim = rotary_order.shape[0]
    blocks = prepare(joined_weight, piece)
    grouped = lax.all_to_all(blocks, BOTH, 0, 0, tiled=True, axis_index_groups=PAIRED)
    moved = grouped.reshape(-1, layers, SLOTS * piece, features // 2)
    moved = lax.all_to_all(moved, "ma", 0, 0, tiled=True)
    query, key, value, peak = finish(moved, turning(rotary_order), norm_gain, dim)
    peak = peak[:, 0].astype(jnp.bfloat16)
    for step in (1, 2, 4, 8):
        peak = jnp.maximum(peak, lax.ppermute(peak, "ma", [(j, j ^ step) for j in range(16)]))
    return query, key, value, peak.astype(jnp.float32)


def solution(mesh):
    return jax.shard_map(
        shards,
        mesh=mesh,
        in_specs=(P(None, "dev", "ma"), P(None, "ma"), P()),
        out_specs=(
            P(None, "dev", "ma"),
            P(None, "dev", "ma"),
            P(None, "dev", "ma"),
            P(None, "dev"),
        ),
        check_vma=False,
    )
```

```python
import jax
import jax.numpy as jnp
import numpy as np
from jax import lax
from jax.experimental import pallas as pl
from jax.experimental.pallas import tpu as pltpu
from jax.sharding import PartitionSpec as P

HEADS = 32
KV_HEADS = 8
GROUP = 4
SLOTS = GROUP + 2
HEAD_TOTAL = HEADS + 2 * KV_HEADS
CHUNKS = 2
SIDE = 4
PLACES = 8


def number(a, y, b, x, core):
    return (a * SIDE + y) * 16 + b * 8 + x * 2 + core


def everywhere():
    for n in range(128):
        i, j = divmod(n, 16)
        yield n, i >> 2, i & 3, j >> 3, (j >> 1) & 3, j & 1


def swap(array):
    pairs = [(n, number(a, y, b, x, core ^ 1)) for n, a, y, b, x, core in everywhere()]
    return lax.ppermute(array, ("dev", "ma"), pairs)


def first_move(array, r, s):
    pairs = [(n, number(a ^ s, (y + r) % SIDE, b ^ s, x, core)) for n, a, y, b, x, core in everywhere()]
    return lax.ppermute(array, ("dev", "ma"), pairs)


def second_move(array, q, s):
    pairs = [(n, number(a, y, b ^ s, (x + q) % SIDE, core)) for n, a, y, b, x, core in everywhere()]
    return lax.ppermute(array, ("dev", "ma"), pairs)


def position():
    dev = lax.axis_index("dev")
    ma = lax.axis_index("ma")
    return dev >> 2, dev & 3, ma >> 3, (ma >> 1) & 3, ma & 1


def picker(piece):
    columns = piece * HEAD_TOTAL
    pick = np.zeros((columns, columns), np.float32)
    for g in range(KV_HEADS):
        for s in range(SLOTS):
            head = g * GROUP + s if s < GROUP else HEADS + (s - GROUP) * KV_HEADS + g
            for d in range(piece):
                pick[(g * SLOTS + s) * piece + d, d * HEAD_TOTAL + head] = 1.0
    return jnp.asarray(pick, jnp.bfloat16)


def prepare_body(place_ref, pick_ref, own_ref, other_ref, *refs):
    out_refs = refs[:PLACES]
    turned_ref = refs[PLACES]
    width = own_ref.shape[1]
    contract = (((1,), (1,)), ((), ()))

    def turned(ref):
        rows = lax.dot_general(pick_ref[...], ref[0], contract, preferred_element_type=jnp.float32)
        return rows.reshape(KV_HEADS * SLOTS, -1, width)

    both = jnp.concatenate([turned(own_ref), turned(other_ref)], axis=1)
    turned_ref[...] = both.reshape(-1, width).astype(jnp.bfloat16)
    rows = turned_ref.shape[0] // KV_HEADS
    a = place_ref[1]
    y = place_ref[2]
    for s in range(2):
        for r in range(SIDE):
            g = (a ^ s) * SIDE + ((y + r) & (SIDE - 1))
            out_refs[s * SIDE + r][0] = turned_ref[pl.ds(pl.multiple_of(g * rows, 16), rows), :]


def prepare(stored, other, place, chunk):
    layers, features, columns = stored.shape
    layers = layers // CHUNKS
    width = features // 2
    rows = 2 * columns // KV_HEADS
    return pl.pallas_call(
        prepare_body,
        grid_spec=pltpu.PrefetchScalarGridSpec(
            num_scalar_prefetch=1,
            grid=(layers,),
            in_specs=[
                pl.BlockSpec((columns, columns), lambda l, place: (0, 0)),
                pl.BlockSpec((1, width, columns), lambda l, place: (chunk * layers + l, place[0], 0)),
                pl.BlockSpec((1, width, columns), lambda l, place: (l, 0, 0)),
            ],
            out_specs=[pl.BlockSpec((1, rows, width), lambda l, place: (l, 0, 0))] * PLACES,
            scratch_shapes=[pltpu.VMEM((2 * columns, width), jnp.bfloat16)],
        ),
        out_shape=[jax.ShapeDtypeStruct((layers, rows, width), jnp.bfloat16)] * PLACES,
        name="prepare",
    )(place, picker(columns // HEAD_TOTAL), stored, other)


def reorder_body(*refs):
    in_refs = refs[:PLACES]
    out_refs = refs[PLACES : 2 * PLACES]
    sems = refs[2 * PLACES]
    a, y, b, x, _ = position()
    flip = a ^ b
    turn = (y - x) & (SIDE - 1)
    for f in range(2):
        for t in range(SIDE):

            @pl.when((flip == f) & (turn == t))
            def _(f=f, t=t):
                copies = []
                for s in range(2):
                    for q in range(SIDE):
                        source = (s ^ f) * SIDE + ((t - q) & (SIDE - 1))
                        k = s * SIDE + q
                        copies.append(pltpu.make_async_copy(in_refs[source], out_refs[k], sems.at[k]))
                for copy in copies:
                    copy.start()
                for copy in copies:
                    copy.wait()


def reorder(buffers):
    spec = pl.BlockSpec(memory_space=pltpu.HBM)
    return pl.pallas_call(
        reorder_body,
        in_specs=[spec] * PLACES,
        out_specs=[spec] * PLACES,
        out_shape=[jax.ShapeDtypeStruct(v.shape, v.dtype) for v in buffers],
        scratch_shapes=[pltpu.SemaphoreType.DMA((PLACES,))],
        name="reorder",
    )(*buffers)


def finish_body(turn_ref, gain_ref, *refs):
    moved_refs = refs[:PLACES]
    query_ref, key_ref, value_ref, peak_ref = refs[-4:]
    _, rows, width = moved_refs[0].shape
    piece = rows // SLOTS
    dim = PLACES * piece
    gain = gain_ref[0]
    for s in range(SLOTS):
        held = jnp.concatenate([ref[0, s * piece : (s + 1) * piece, :] for ref in moved_refs], axis=0)
        turned = jnp.dot(turn_ref[s // (SLOTS - 1)], held, preferred_element_type=jnp.float32)
        scaled = (turned * gain).astype(jnp.bfloat16)
        if s < GROUP:
            query_ref[0, s * dim : (s + 1) * dim, :] = scaled
        elif s == GROUP:
            key_ref[0] = scaled
        else:
            value_ref[0] = scaled
        size = jnp.abs(scaled.astype(jnp.float32))
        size = jnp.maximum(size[:, :128], size[:, 128:])
        peak_ref[0, :, s * dim : (s + 1) * dim] = jnp.max(size.T, axis=0, keepdims=True)


def finish(moved, turn, gain, chunk, earlier):
    layers, rows, width = moved[0].shape
    dim = turn.shape[1]
    whole = layers * CHUNKS

    def at(*shape):
        return pl.BlockSpec((1, *shape), lambda l: (chunk * layers + l, 0, 0))

    held = [pl.BlockSpec((1, rows, width), lambda l: (l, 0, 0))] * PLACES
    shapes = [
        ((GROUP * dim, width), jnp.bfloat16),
        ((dim, width), jnp.bfloat16),
        ((dim, width), jnp.bfloat16),
        ((1, SLOTS * dim), jnp.float32),
    ]
    return pl.pallas_call(
        finish_body,
        grid=(layers,),
        in_specs=[pl.BlockSpec((2, dim, dim), lambda l: (0, 0, 0)), at(1, width)]
        + held
        + [pl.BlockSpec(memory_space=pltpu.HBM)] * len(earlier),
        out_specs=[at(*shape) for shape, _ in shapes],
        out_shape=[jax.ShapeDtypeStruct((whole, *shape), kind) for shape, kind in shapes],
        input_output_aliases={2 + PLACES + k: k for k in range(len(earlier))},
        name="finish",
    )(turn, gain, *moved, *earlier)


def turning(rotary_order):
    dim = rotary_order.shape[0]
    piece = dim // PLACES
    a, _, _, x, core = position()
    place = jnp.arange(dim, dtype=jnp.int32)
    s = place // (SIDE * piece)
    q = (place // piece) & (SIDE - 1)
    t = place & (piece - 1)
    holds = ((s ^ a) * SIDE + ((x - q) & (SIDE - 1))) * piece + (t ^ (core * (piece // 2)))
    orders = jnp.stack([rotary_order, place])
    return (orders[:, :, None] == holds[None, None, :]).astype(jnp.bfloat16)


STAGE = ((1, 0), (3, 0), (2, 0), (0, 1), (1, 1), (3, 1), (2, 1))


def staged(buffers, move):
    out = list(buffers)
    for step, s in STAGE:
        k = s * SIDE + step
        out[k] = move(buffers[k], step, s)
    return out


def shards(joined_weight, norm_gain, rotary_order):
    layers, features, columns = joined_weight.shape
    width = features // 2
    count = layers // CHUNKS
    a, y, _, _, core = position()
    place = jnp.stack([core, a, y]).astype(jnp.int32)
    turn = turning(rotary_order)
    gain = norm_gain[:, None, :]
    outs = []
    moved = []
    for chunk in range(CHUNKS):
        theirs = lax.dynamic_slice(
            joined_weight, (chunk * count, (1 - core) * width, 0), (count, width, columns)
        )
        blocks = prepare(joined_weight, swap(theirs), place, chunk)
        moved.append(staged(blocks, first_move))
    for chunk in range(CHUNKS):
        arrived = staged(reorder(moved[chunk]), second_move)
        outs = finish(arrived, turn, gain, chunk, outs)
    query, key, value, peak = outs
    peak = peak[:, 0].astype(jnp.bfloat16)
    for step in (1, 2, 4, 8):
        peak = jnp.maximum(peak, lax.ppermute(peak, "ma", [(j, j ^ step) for j in range(16)]))
    return query, key, value, peak.astype(jnp.float32)


def solution(mesh):
    return jax.shard_map(
        shards,
        mesh=mesh,
        in_specs=(P(None, "dev", "ma"), P(None, "ma"), P()),
        out_specs=(
            P(None, "dev", "ma"),
            P(None, "dev", "ma"),
            P(None, "dev", "ma"),
            P(None, "dev"),
        ),
        check_vma=False,
    )
```

```python
import jax
import jax.numpy as jnp
import numpy as np
from jax import lax
from jax.experimental import pallas as pl
from jax.experimental.pallas import tpu as pltpu
from jax.sharding import PartitionSpec as P

HEADS = 32
KV_HEADS = 8
GROUP = 4
SLOTS = GROUP + 2
HEAD_TOTAL = HEADS + 2 * KV_HEADS
CHUNKS = 2
SIDE = 4
PLACES = 8


def number(a, y, b, x, core):
    return (a * SIDE + y) * 16 + b * 8 + x * 2 + core


def everywhere():
    for n in range(128):
        i, j = divmod(n, 16)
        yield n, i >> 2, i & 3, j >> 3, (j >> 1) & 3, j & 1


def swap(array):
    pairs = [(n, number(a, y, b, x, core ^ 1)) for n, a, y, b, x, core in everywhere()]
    return lax.ppermute(array, ("dev", "ma"), pairs)


def first_move(array, r, s):
    pairs = [(n, number(a ^ s, (y + r) % SIDE, b ^ s, x, core)) for n, a, y, b, x, core in everywhere()]
    return lax.ppermute(array, ("dev", "ma"), pairs)


def second_move(array, q, s):
    pairs = [(n, number(a, y, b ^ s, (x + q) % SIDE, core)) for n, a, y, b, x, core in everywhere()]
    return lax.ppermute(array, ("dev", "ma"), pairs)


def position():
    dev = lax.axis_index("dev")
    ma = lax.axis_index("ma")
    return dev >> 2, dev & 3, ma >> 3, (ma >> 1) & 3, ma & 1


def picker(piece):
    columns = piece * HEAD_TOTAL
    pick = np.zeros((columns, columns), np.float32)
    for g in range(KV_HEADS):
        for s in range(SLOTS):
            head = g * GROUP + s if s < GROUP else HEADS + (s - GROUP) * KV_HEADS + g
            for d in range(piece):
                pick[(g * SLOTS + s) * piece + d, d * HEAD_TOTAL + head] = 1.0
    return jnp.asarray(pick, jnp.bfloat16)


def prepare_body(place_ref, pick_ref, own_ref, other_ref, *refs):
    out_refs = refs[:PLACES]
    turned_ref = refs[PLACES]
    width = own_ref.shape[1]
    contract = (((1,), (1,)), ((), ()))

    def turned(ref):
        rows = lax.dot_general(pick_ref[...], ref[0], contract, preferred_element_type=jnp.float32)
        return rows.reshape(KV_HEADS * SLOTS, -1, width)

    both = jnp.concatenate([turned(own_ref), turned(other_ref)], axis=1)
    turned_ref[...] = both.reshape(-1, width).astype(jnp.bfloat16)
    rows = turned_ref.shape[0] // KV_HEADS
    a = place_ref[1]
    y = place_ref[2]
    for s in range(2):
        for r in range(SIDE):
            g = (a ^ s) * SIDE + ((y + r) & (SIDE - 1))
            out_refs[s * SIDE + r][0] = turned_ref[pl.ds(pl.multiple_of(g * rows, 16), rows), :]


def prepare(stored, other, place, chunk):
    layers, features, columns = stored.shape
    layers = layers // CHUNKS
    width = features // 2
    rows = 2 * columns // KV_HEADS
    return pl.pallas_call(
        prepare_body,
        grid_spec=pltpu.PrefetchScalarGridSpec(
            num_scalar_prefetch=1,
            grid=(layers,),
            in_specs=[
                pl.BlockSpec((columns, columns), lambda l, place: (0, 0)),
                pl.BlockSpec((1, width, columns), lambda l, place: (chunk * layers + l, place[0], 0)),
                pl.BlockSpec((1, width, columns), lambda l, place: (l, 0, 0)),
            ],
            out_specs=[pl.BlockSpec((1, rows, width), lambda l, place: (l, 0, 0))] * PLACES,
            scratch_shapes=[pltpu.VMEM((2 * columns, width), jnp.bfloat16)],
        ),
        out_shape=[jax.ShapeDtypeStruct((layers, rows, width), jnp.bfloat16)] * PLACES,
        name="prepare",
    )(place, picker(columns // HEAD_TOTAL), stored, other)


def reorder_body(*refs):
    in_refs = refs[:PLACES]
    out_refs = refs[PLACES : 2 * PLACES]
    held_ref, in_sems, out_sems = refs[2 * PLACES :]
    a, y, b, x, _ = position()
    flip = a ^ b
    turn = (y - x) & (SIDE - 1)
    for f in range(2):
        for t in range(SIDE):

            @pl.when((flip == f) & (turn == t))
            def _(f=f, t=t):
                for s in range(2):
                    for q in range(SIDE):
                        source = (s ^ f) * SIDE + ((t - q) & (SIDE - 1))
                        k = s * SIDE + q
                        pltpu.make_async_copy(in_refs[source], held_ref.at[k], in_sems.at[k]).start()

    for k in range(PLACES):
        pltpu.make_async_copy(in_refs[k], held_ref.at[k], in_sems.at[k]).wait()
        pltpu.make_async_copy(held_ref.at[k], out_refs[k], out_sems.at[k]).start()
    for k in range(PLACES):
        pltpu.make_async_copy(held_ref.at[k], out_refs[k], out_sems.at[k]).wait()


def reorder(buffers):
    spec = pl.BlockSpec(memory_space=pltpu.HBM)
    shape = buffers[0].shape
    return pl.pallas_call(
        reorder_body,
        in_specs=[spec] * PLACES,
        out_specs=[spec] * PLACES,
        out_shape=[jax.ShapeDtypeStruct(shape, v.dtype) for v in buffers],
        scratch_shapes=[
            pltpu.VMEM((PLACES, *shape), jnp.bfloat16),
            pltpu.SemaphoreType.DMA((PLACES,)),
            pltpu.SemaphoreType.DMA((PLACES,)),
        ],
        name="reorder",
    )(*buffers)


def finish_body(turn_ref, gain_ref, *refs):
    moved_refs = refs[:PLACES]
    query_ref, key_ref, value_ref, peak_ref = refs[-4:]
    _, rows, width = moved_refs[0].shape
    piece = rows // SLOTS
    dim = PLACES * piece
    gain = gain_ref[0]
    for s in range(SLOTS):
        held = jnp.concatenate([ref[0, s * piece : (s + 1) * piece, :] for ref in moved_refs], axis=0)
        turned = jnp.dot(turn_ref[s // (SLOTS - 1)], held, preferred_element_type=jnp.float32)
        scaled = (turned * gain).astype(jnp.bfloat16)
        if s < GROUP:
            query_ref[0, s * dim : (s + 1) * dim, :] = scaled
        elif s == GROUP:
            key_ref[0] = scaled
        else:
            value_ref[0] = scaled
        size = jnp.abs(scaled.astype(jnp.float32))
        size = jnp.maximum(size[:, :128], size[:, 128:])
        peak_ref[0, :, s * dim : (s + 1) * dim] = jnp.max(size.T, axis=0, keepdims=True)


def finish(moved, turn, gain, chunk, earlier):
    layers, rows, width = moved[0].shape
    dim = turn.shape[1]
    whole = layers * CHUNKS

    def at(*shape):
        return pl.BlockSpec((1, *shape), lambda l: (chunk * layers + l, 0, 0))

    held = [pl.BlockSpec((1, rows, width), lambda l: (l, 0, 0))] * PLACES
    shapes = [
        ((GROUP * dim, width), jnp.bfloat16),
        ((dim, width), jnp.bfloat16),
        ((dim, width), jnp.bfloat16),
        ((1, SLOTS * dim), jnp.float32),
    ]
    return pl.pallas_call(
        finish_body,
        grid=(layers,),
        in_specs=[pl.BlockSpec((2, dim, dim), lambda l: (0, 0, 0)), at(1, width)]
        + held
        + [pl.BlockSpec(memory_space=pltpu.HBM)] * len(earlier),
        out_specs=[at(*shape) for shape, _ in shapes],
        out_shape=[jax.ShapeDtypeStruct((whole, *shape), kind) for shape, kind in shapes],
        input_output_aliases={2 + PLACES + k: k for k in range(len(earlier))},
        name="finish",
    )(turn, gain, *moved, *earlier)


def turning(rotary_order):
    dim = rotary_order.shape[0]
    piece = dim // PLACES
    a, _, _, x, core = position()
    place = jnp.arange(dim, dtype=jnp.int32)
    s = place // (SIDE * piece)
    q = (place // piece) & (SIDE - 1)
    t = place & (piece - 1)
    holds = ((s ^ a) * SIDE + ((x - q) & (SIDE - 1))) * piece + (t ^ (core * (piece // 2)))
    orders = jnp.stack([rotary_order, place])
    return (orders[:, :, None] == holds[None, None, :]).astype(jnp.bfloat16)


STAGE = ((1, 0), (3, 0), (2, 0), (0, 1), (1, 1), (3, 1), (2, 1))


def staged(buffers, move):
    out = list(buffers)
    for step, s in STAGE:
        k = s * SIDE + step
        out[k] = move(buffers[k], step, s)
    return out


def shards(joined_weight, norm_gain, rotary_order):
    layers, features, columns = joined_weight.shape
    width = features // 2
    count = layers // CHUNKS
    a, y, _, _, core = position()
    place = jnp.stack([core, a, y]).astype(jnp.int32)
    turn = turning(rotary_order)
    gain = norm_gain[:, None, :]
    outs = []
    moved = []
    for chunk in range(CHUNKS):
        theirs = lax.dynamic_slice(
            joined_weight, (chunk * count, (1 - core) * width, 0), (count, width, columns)
        )
        blocks = prepare(joined_weight, swap(theirs), place, chunk)
        moved.append(staged(blocks, first_move))
    for chunk in range(CHUNKS):
        arrived = staged(reorder(moved[chunk]), second_move)
        outs = finish(arrived, turn, gain, chunk, outs)
    query, key, value, peak = outs
    peak = peak[:, 0].astype(jnp.bfloat16)
    for step in (1, 2, 4, 8):
        peak = jnp.maximum(peak, lax.ppermute(peak, "ma", [(j, j ^ step) for j in range(16)]))
    return query, key, value, peak.astype(jnp.float32)


def solution(mesh):
    return jax.shard_map(
        shards,
        mesh=mesh,
        in_specs=(P(None, "dev", "ma"), P(None, "ma"), P()),
        out_specs=(
            P(None, "dev", "ma"),
            P(None, "dev", "ma"),
            P(None, "dev", "ma"),
            P(None, "dev"),
        ),
        check_vma=False,
    )
```

```python
import jax
import jax.numpy as jnp
import numpy as np
from jax import lax
from jax.experimental import pallas as pl
from jax.experimental.pallas import tpu as pltpu
from jax.sharding import PartitionSpec as P

HEADS = 32
KV_HEADS = 8
GROUP = 4
SLOTS = GROUP + 2
HEAD_TOTAL = HEADS + 2 * KV_HEADS
CHUNKS = 2
SIDE = 4
PLACES = 8


def number(a, y, b, x, core):
    return (a * SIDE + y) * 16 + b * 8 + x * 2 + core


def everywhere():
    for n in range(128):
        i, j = divmod(n, 16)
        yield n, i >> 2, i & 3, j >> 3, (j >> 1) & 3, j & 1


def swap(array):
    pairs = [(n, number(a, y, b, x, core ^ 1)) for n, a, y, b, x, core in everywhere()]
    return lax.ppermute(array, ("dev", "ma"), pairs)


def first_move(array, r, chunk):
    pairs = []
    for n, a, y, b, x, core in everywhere():
        s = chunk ^ core ^ a ^ b
        pairs.append((n, number(a ^ s, (y + r) % SIDE, b ^ s, x, core)))
    return lax.ppermute(array, ("dev", "ma"), pairs)


def second_move(array, q, chunk):
    pairs = []
    for n, a, y, b, x, core in everywhere():
        s = chunk ^ core
        pairs.append((n, number(a, y, b ^ s, (x + q) % SIDE, core)))
    return lax.ppermute(array, ("dev", "ma"), pairs)


def position():
    dev = lax.axis_index("dev")
    ma = lax.axis_index("ma")
    return dev >> 2, dev & 3, ma >> 3, (ma >> 1) & 3, ma & 1


def picker(piece):
    columns = piece * HEAD_TOTAL
    pick = np.zeros((columns, columns), np.float32)
    for g in range(KV_HEADS):
        for s in range(SLOTS):
            head = g * GROUP + s if s < GROUP else HEADS + (s - GROUP) * KV_HEADS + g
            for d in range(piece):
                pick[(g * SLOTS + s) * piece + d, d * HEAD_TOTAL + head] = 1.0
    return jnp.asarray(pick.reshape(2, columns // 2, columns), jnp.bfloat16)


def prepare_body(place_ref, pick_ref, own_ref, other_ref, *refs):
    out_refs = refs[:SIDE]
    turned_ref = refs[SIDE]
    width = own_ref.shape[1]
    contract = (((1,), (1,)), ((), ()))

    def turned(ref):
        rows = lax.dot_general(pick_ref[0], ref[0], contract, preferred_element_type=jnp.float32)
        return rows.reshape(SIDE * SLOTS, -1, width)

    both = jnp.concatenate([turned(own_ref), turned(other_ref)], axis=1)
    turned_ref[...] = both.reshape(-1, width).astype(jnp.bfloat16)
    rows = turned_ref.shape[0] // SIDE
    y = place_ref[2]
    for r in range(SIDE):
        target = (y + r) & (SIDE - 1)
        out_refs[r][0] = turned_ref[pl.ds(pl.multiple_of(target * rows, 16), rows), :]


def prepare(stored, other, place):
    layers, features, columns = stored.shape
    width = features // 2
    rows = columns // SIDE
    return pl.pallas_call(
        prepare_body,
        grid_spec=pltpu.PrefetchScalarGridSpec(
            num_scalar_prefetch=1,
            grid=(layers,),
            in_specs=[
                pl.BlockSpec((1, columns // 2, columns), lambda l, place: (place[1], 0, 0)),
                pl.BlockSpec((1, width, columns), lambda l, place: (l, place[0], 0)),
                pl.BlockSpec((1, width, columns), lambda l, place: (l, 0, 0)),
            ],
            out_specs=[pl.BlockSpec((1, rows, width), lambda l, place: (l, 0, 0))] * SIDE,
            scratch_shapes=[pltpu.VMEM((columns, width), jnp.bfloat16)],
        ),
        out_shape=[jax.ShapeDtypeStruct((layers, rows, width), jnp.bfloat16)] * SIDE,
        name="prepare",
    )(place, picker(columns // HEAD_TOTAL), stored, other)


def reorder_body(*refs):
    in_refs = refs[:SIDE]
    out_refs = refs[SIDE : 2 * SIDE]
    held_ref, in_sems, out_sems = refs[2 * SIDE :]
    _, y, _, x, _ = position()
    turn = (y - x) & (SIDE - 1)
    for t in range(SIDE):

        @pl.when(turn == t)
        def _(t=t):
            for q in range(SIDE):
                source = in_refs[(t - q) & (SIDE - 1)]
                pltpu.make_async_copy(source, held_ref.at[q], in_sems.at[q]).start()

    for q in range(SIDE):
        pltpu.make_async_copy(in_refs[q], held_ref.at[q], in_sems.at[q]).wait()
        pltpu.make_async_copy(held_ref.at[q], out_refs[q], out_sems.at[q]).start()
    for q in range(SIDE):
        pltpu.make_async_copy(held_ref.at[q], out_refs[q], out_sems.at[q]).wait()


def reorder(buffers):
    spec = pl.BlockSpec(memory_space=pltpu.HBM)
    shape = buffers[0].shape
    return pl.pallas_call(
        reorder_body,
        in_specs=[spec] * SIDE,
        out_specs=[spec] * SIDE,
        out_shape=[jax.ShapeDtypeStruct(shape, v.dtype) for v in buffers],
        scratch_shapes=[
            pltpu.VMEM((SIDE, *shape), jnp.bfloat16),
            pltpu.SemaphoreType.DMA((SIDE,)),
            pltpu.SemaphoreType.DMA((SIDE,)),
        ],
        name="reorder",
    )(*buffers)


def finish_body(turn_ref, gain_ref, *refs):
    moved_refs = refs[:PLACES]
    query_ref, key_ref, value_ref, peak_ref = refs[-4:]
    _, rows, width = moved_refs[0].shape
    piece = rows // SLOTS
    dim = PLACES * piece
    gain = gain_ref[0]
    for s in range(SLOTS):
        held = jnp.concatenate([ref[0, s * piece : (s + 1) * piece, :] for ref in moved_refs], axis=0)
        turned = jnp.dot(turn_ref[s // (SLOTS - 1)], held, preferred_element_type=jnp.float32)
        scaled = (turned * gain).astype(jnp.bfloat16)
        if s < GROUP:
            query_ref[0, s * dim : (s + 1) * dim, :] = scaled
        elif s == GROUP:
            key_ref[0] = scaled
        else:
            value_ref[0] = scaled
        size = jnp.abs(scaled.astype(jnp.float32))
        size = jnp.maximum(size[:, :128], size[:, 128:])
        peak_ref[0, :, s * dim : (s + 1) * dim] = jnp.max(size.T, axis=0, keepdims=True)


def finish(moved, turn, gain):
    layers, rows, width = moved[0].shape
    dim = turn.shape[1]

    def at(*shape):
        return pl.BlockSpec((1, *shape), lambda l: (l, 0, 0))

    shapes = [
        ((GROUP * dim, width), jnp.bfloat16),
        ((dim, width), jnp.bfloat16),
        ((dim, width), jnp.bfloat16),
        ((1, SLOTS * dim), jnp.float32),
    ]
    return pl.pallas_call(
        finish_body,
        grid=(layers,),
        in_specs=[pl.BlockSpec((2, dim, dim), lambda l: (0, 0, 0)), at(1, width)]
        + [at(rows, width)] * PLACES,
        out_specs=[at(*shape) for shape, _ in shapes],
        out_shape=[jax.ShapeDtypeStruct((layers, *shape), kind) for shape, kind in shapes],
        name="finish",
    )(turn, gain, *moved)


def turning(rotary_order):
    dim = rotary_order.shape[0]
    piece = dim // PLACES
    a, _, _, x, core = position()
    place = jnp.arange(dim, dtype=jnp.int32)
    chunk = place // (SIDE * piece)
    q = (place // piece) & (SIDE - 1)
    t = place & (piece - 1)
    upper = chunk ^ core ^ a
    holds = (upper * SIDE + ((x - q) & (SIDE - 1))) * piece + (t ^ (core * (piece // 2)))
    orders = jnp.stack([rotary_order, place])
    return (orders[:, :, None] == holds[None, None, :]).astype(jnp.bfloat16)


STEPS = (1, 3, 2, 0)


def staged(buffers, move, chunk):
    out = list(buffers)
    for step in STEPS:
        out[step] = move(buffers[step], step, chunk)
    return out


def shards(joined_weight, norm_gain, rotary_order):
    layers, features, columns = joined_weight.shape
    width = features // 2
    _, y, b, _, core = position()
    turn = turning(rotary_order)
    theirs = lax.dynamic_slice(joined_weight, (0, (1 - core) * width, 0), (layers, width, columns))
    theirs = swap(theirs)
    moved = []
    for chunk in range(CHUNKS):
        place = jnp.stack([core, b ^ chunk ^ core, y]).astype(jnp.int32)
        moved.append(staged(prepare(joined_weight, theirs, place), first_move, chunk))
    arrived = []
    for chunk in range(CHUNKS):
        arrived += staged(reorder(moved[chunk]), second_move, chunk)
    query, key, value, peak = finish(arrived, turn, norm_gain[:, None, :])
    peak = peak[:, 0].astype(jnp.bfloat16)
    for step in (1, 2, 4, 8):
        peak = jnp.maximum(peak, lax.ppermute(peak, "ma", [(j, j ^ step) for j in range(16)]))
    return query, key, value, peak.astype(jnp.float32)


def solution(mesh):
    return jax.shard_map(
        shards,
        mesh=mesh,
        in_specs=(P(None, "dev", "ma"), P(None, "ma"), P()),
        out_specs=(
            P(None, "dev", "ma"),
            P(None, "dev", "ma"),
            P(None, "dev", "ma"),
            P(None, "dev"),
        ),
        check_vma=False,
    )
```

```python
import functools

import jax
import jax.numpy as jnp
import numpy as np
from jax import lax
from jax.experimental import pallas as pl
from jax.experimental.pallas import tpu as pltpu
from jax.sharding import PartitionSpec as P


HEADS = 32
KV_HEADS = 8
GROUP = 4
SLOTS = GROUP + 2
HEAD_TOTAL = HEADS + 2 * KV_HEADS
SIZES = (4, 4)
WHOLE = (False, True)
SIDE = 4
PLACES = 8


def number(a, y, b, x, core):
    return (a * SIDE + y) * 16 + b * 8 + x * 2 + core


def everywhere():
    for n in range(128):
        i, j = divmod(n, 16)
        yield n, i >> 2, i & 3, j >> 3, (j >> 1) & 3, j & 1


def swap(array):
    pairs = [(n, number(a, y, b, x, core ^ 1)) for n, a, y, b, x, core in everywhere()]
    return lax.ppermute(array, ("dev", "ma"), pairs)


def gain_move(gain):
    pairs = [(n, number(b, x, a, y, core)) for n, a, y, b, x, core in everywhere()]
    return lax.ppermute(gain, ("dev", "ma"), pairs)


def first_move(array, r, s):
    pairs = [(n, number(a ^ s, (y + r) % SIDE, b ^ s, x, core)) for n, a, y, b, x, core in everywhere()]
    return lax.ppermute(array, ("dev", "ma"), pairs)


def second_move(array, q, s):
    pairs = [(n, number(a, y, b ^ s, (x + q) % SIDE, core)) for n, a, y, b, x, core in everywhere()]
    return lax.ppermute(array, ("dev", "ma"), pairs)


def position():
    dev = lax.axis_index("dev")
    ma = lax.axis_index("ma")
    return dev >> 2, dev & 3, ma >> 3, (ma >> 1) & 3, ma & 1


def picker(piece):
    columns = piece * HEAD_TOTAL
    pick = np.zeros((columns, columns), np.float32)
    for g in range(KV_HEADS):
        for s in range(SLOTS):
            head = g * GROUP + s if s < GROUP else HEADS + (s - GROUP) * KV_HEADS + g
            for d in range(piece):
                pick[(g * SLOTS + s) * piece + d, d * HEAD_TOTAL + head] = 1.0
    return jnp.asarray(pick, jnp.bfloat16)


def prepare_body(first, place_ref, pick_ref, gain_ref, own_ref, other_ref, *refs):
    out_refs = refs[:-1]
    turned_ref = refs[-1]
    width = own_ref.shape[1]
    contract = (((1,), (1,)), ((), ()))

    def turned(ref):
        rows = lax.dot_general(pick_ref[...], ref[0], contract, preferred_element_type=jnp.float32)
        return rows.reshape(KV_HEADS * SLOTS, -1, width)

    both = jnp.concatenate([turned(own_ref), turned(other_ref)], axis=1)
    both = both.reshape(-1, width)
    if len(out_refs) == 1:
        both = both * gain_ref[pl.ds(first + pl.program_id(0), 1), :]
    turned_ref[...] = both.astype(jnp.bfloat16)
    rows = turned_ref.shape[0] // KV_HEADS
    if len(out_refs) == 1:
        out_refs[0][:, 0] = turned_ref[...].reshape(KV_HEADS, rows, width)
        return
    a = place_ref[1]
    y = place_ref[2]
    for s in range(2):
        for r in range(SIDE):
            g = (a ^ s) * SIDE + ((y + r) & (SIDE - 1))
            out_refs[s * SIDE + r][0] = turned_ref[pl.ds(pl.multiple_of(g * rows, 16), rows), :]


def prepare(stored, other, gain, place, first, whole):
    _, features, columns = stored.shape
    layers = other.shape[0]
    width = features // 2
    rows = 2 * columns // KV_HEADS
    if whole:
        out_specs = [pl.BlockSpec((PLACES, 1, rows, width), lambda l, place: (0, l, 0, 0))]
        out_shape = [jax.ShapeDtypeStruct((PLACES, layers, rows, width), jnp.bfloat16)]
    else:
        out_specs = [pl.BlockSpec((1, rows, width), lambda l, place: (l, 0, 0))] * PLACES
        out_shape = [jax.ShapeDtypeStruct((layers, rows, width), jnp.bfloat16)] * PLACES
    return pl.pallas_call(
        functools.partial(prepare_body, first),
        grid_spec=pltpu.PrefetchScalarGridSpec(
            num_scalar_prefetch=1,
            grid=(layers,),
            in_specs=[
                pl.BlockSpec((columns, columns), lambda l, place: (0, 0)),
                pl.BlockSpec(gain.shape, lambda l, place: (0, 0)),
                pl.BlockSpec((1, width, columns), lambda l, place: (first + l, place[0], 0)),
                pl.BlockSpec((1, width, columns), lambda l, place: (l, 0, 0)),
            ],
            out_specs=out_specs,
            scratch_shapes=[pltpu.VMEM((2 * columns, width), jnp.bfloat16)],
        ),
        out_shape=out_shape,
        name="prepare",
    )(place, picker(columns // HEAD_TOTAL), gain, stored, other)


def reorder_body(*refs):
    in_refs = refs[:PLACES]
    out_refs = refs[PLACES : 2 * PLACES]
    held_ref, in_sems, out_sems = refs[2 * PLACES :]
    a, y, b, x, _ = position()
    flip = a ^ b
    turn = (y - x) & (SIDE - 1)
    for f in range(2):
        for t in range(SIDE):

            @pl.when((flip == f) & (turn == t))
            def _(f=f, t=t):
                for s in range(2):
                    for q in range(SIDE):
                        source = (s ^ f) * SIDE + ((t - q) & (SIDE - 1))
                        k = s * SIDE + q
                        pltpu.make_async_copy(in_refs[source], held_ref.at[k], in_sems.at[k]).start()

    for k in range(PLACES):
        pltpu.make_async_copy(in_refs[k], held_ref.at[k], in_sems.at[k]).wait()
        pltpu.make_async_copy(held_ref.at[k], out_refs[k], out_sems.at[k]).start()
    for k in range(PLACES):
        pltpu.make_async_copy(held_ref.at[k], out_refs[k], out_sems.at[k]).wait()


def reorder(buffers):
    spec = pl.BlockSpec(memory_space=pltpu.HBM)
    shape = buffers[0].shape
    return pl.pallas_call(
        reorder_body,
        in_specs=[spec] * PLACES,
        out_specs=[spec] * PLACES,
        out_shape=[jax.ShapeDtypeStruct(shape, v.dtype) for v in buffers],
        scratch_shapes=[
            pltpu.VMEM((PLACES, *shape), jnp.bfloat16),
            pltpu.SemaphoreType.DMA((PLACES,)),
            pltpu.SemaphoreType.DMA((PLACES,)),
        ],
        name="reorder",
    )(*buffers)


def peak_body(*refs):
    moved_refs, out_ref = refs[:-1], refs[-1]
    _, _, width = moved_refs[0].shape
    for u in range(2):
        size = jnp.abs(moved_refs[u * SIDE][...])
        for v in range(1, SIDE):
            size = jnp.maximum(size, jnp.abs(moved_refs[u * SIDE + v][...]))
        size = size.reshape(-1, width).astype(jnp.float32)
        size = jnp.maximum(size[:, :128], size[:, 128:])
        out_ref[u : u + 1, :] = jnp.max(size.T, axis=0, keepdims=True)


def peaks(moved):
    layers, rows, width = moved[0].shape[-3:]
    if len(moved) == 1:
        held = [
            pl.BlockSpec((None, layers, rows, width), lambda l, k=k: (k, 0, 0, 0)) for k in range(PLACES)
        ]
        moved = moved * PLACES
    else:
        held = [pl.BlockSpec((layers, rows, width), lambda l: (0, 0, 0))] * PLACES
    return pl.pallas_call(
        peak_body,
        grid=(1,),
        in_specs=held,
        out_specs=pl.BlockSpec((2, layers * rows), lambda l: (0, 0)),
        out_shape=jax.ShapeDtypeStruct((2, layers * rows), jnp.float32),
        name="peaks",
    )(*moved)


def placed_peaks(found, whole):
    a, _, b, x, core = position()
    found = found.reshape(2, -1, SLOTS, 2, PLACES)
    found = jnp.where(core == 1, found[:, :, :, ::-1], found)
    u = jnp.arange(2)[:, None]
    upper = u ^ a ^ b if whole else u ^ a
    here = jnp.arange(PLACES)[None, :] == upper * SIDE + x
    spread = jnp.where(here[:, None, None, :, None, None], found[:, :, :, None], 0.0)
    return spread.max(0).reshape(found.shape[1], -1).astype(jnp.bfloat16)


def finish_body(turn_ref, gain_ref, first, *refs):
    moved_refs = refs[:PLACES]
    outs = refs[PLACES:]
    if gain_ref is None:
        query_ref, key_ref, value_ref = outs[-3:]
    else:
        query_ref, key_ref, value_ref, peak_ref = outs[-4:]
    _, rows, _ = moved_refs[0].shape
    piece = rows // SLOTS
    dim = PLACES * piece
    for s in range(SLOTS):
        held = jnp.concatenate([ref[0, s * piece : (s + 1) * piece, :] for ref in moved_refs], axis=0)
        turned = jnp.dot(turn_ref[s // (SLOTS - 1)], held, preferred_element_type=jnp.float32)
        if gain_ref is not None:
            turned = turned * gain_ref[pl.ds(first + pl.program_id(0), 1), :]
        turned = turned.astype(jnp.bfloat16)
        if s < GROUP:
            query_ref[0, s * dim : (s + 1) * dim, :] = turned
        elif s == GROUP:
            key_ref[0] = turned
        else:
            value_ref[0] = turned
        if gain_ref is not None:
            size = jnp.abs(turned.astype(jnp.float32))
            size = jnp.maximum(size[:, :128], size[:, 128:])
            peak_ref[0, :, s * dim : (s + 1) * dim] = jnp.max(size.T, axis=0, keepdims=True)


def plain_body(turn_ref, *refs):
    finish_body(turn_ref, None, 0, *refs)


def scaled_body(first, turn_ref, gain_ref, *refs):
    finish_body(turn_ref, gain_ref, first, *refs)


def finish(moved, turn, gain, whole, first, earlier):
    layers, rows, width = moved[0].shape[-3:]
    dim = turn.shape[1]

    def at(*shape):
        return pl.BlockSpec((1, *shape), lambda l: (first + l, 0, 0))

    shapes = [
        ((GROUP * dim, width), jnp.bfloat16),
        ((dim, width), jnp.bfloat16),
        ((dim, width), jnp.bfloat16),
    ]
    out_specs = [at(*shape) for shape, _ in shapes]
    out_shape = [jax.ShapeDtypeStruct((whole, *shape), kind) for shape, kind in shapes]
    before = [turn]
    in_specs = [pl.BlockSpec((2, dim, dim), lambda l: (0, 0, 0))]
    body = plain_body
    if gain is not None:
        body = functools.partial(scaled_body, first)
        before.append(gain)
        in_specs.append(pl.BlockSpec(gain.shape, lambda l: (0, 0)))
        out_specs.append(pl.BlockSpec((1, 1, SLOTS * dim), lambda l: (l, 0, 0)))
        out_shape.append(jax.ShapeDtypeStruct((layers, 1, SLOTS * dim), jnp.float32))
    if len(moved) == 1:
        held = [
            pl.BlockSpec((None, 1, rows, width), lambda l, k=k: (k, l, 0, 0)) for k in range(PLACES)
        ]
        moved = moved * PLACES
    else:
        held = [pl.BlockSpec((1, rows, width), lambda l: (l, 0, 0))] * PLACES
    shapes = [
        ((GROUP * dim, width), jnp.bfloat16),
        ((dim, width), jnp.bfloat16),
        ((dim, width), jnp.bfloat16),
    ]
    return pl.pallas_call(
        body,
        grid=(layers,),
        in_specs=in_specs + held + [pl.BlockSpec(memory_space=pltpu.HBM)] * len(earlier),
        out_specs=out_specs,
        out_shape=out_shape,
        input_output_aliases={len(before) + PLACES + k: k for k in range(len(earlier))},
        name="finish",
    )(*before, *moved, *earlier)


def turning(rotary_order, whole):
    dim = rotary_order.shape[0]
    piece = dim // PLACES
    a, _, b, x, core = position()
    place = jnp.arange(dim, dtype=jnp.int32)
    u = place // (SIDE * piece)
    v = (place // piece) & (SIDE - 1)
    t = place & (piece - 1)
    high, low = (u ^ a ^ b, v) if whole else (u ^ a, (x - v) & (SIDE - 1))
    holds = (high * SIDE + low) * piece + (t ^ (core * (piece // 2)))
    orders = jnp.stack([rotary_order, place])
    return (orders[:, :, None] == holds[None, None, :]).astype(jnp.bfloat16)


FIRST_GROUPS = [
    [number(a, y, a ^ key, x, core) for a in range(2) for y in range(SIDE)]
    for key in range(2)
    for x in range(SIDE)
    for core in range(2)
]
SECOND_GROUPS = [
    [number(a, y, b, x, core) for b in range(2) for x in range(SIDE)]
    for a in range(2)
    for y in range(SIDE)
    for core in range(2)
]


def exchange(array, groups):
    return lax.all_to_all(array, ("dev", "ma"), 0, 0, tiled=True, axis_index_groups=groups)


STAGE = ((1, 0), (3, 0), (2, 0), (0, 1), (1, 1), (3, 1), (2, 1))


def staged(buffers, move):
    out = list(buffers)
    for step, s in STAGE:
        k = s * SIDE + step
        out[k] = move(buffers[k], step, s)
    return out


def shards(joined_weight, norm_gain, rotary_order):
    layers, features, columns = joined_weight.shape
    width = features // 2
    dim = rotary_order.shape[0]
    a, y, _, _, core = position()
    place = jnp.stack([core, a, y]).astype(jnp.int32)
    turns = [turning(rotary_order, False), turning(rotary_order, True)]
    firsts = [sum(SIZES[:k]) for k in range(len(SIZES))]
    gain = gain_move(norm_gain)
    moved = []
    for first, size, whole in zip(firsts, SIZES, WHOLE):
        theirs = lax.dynamic_slice(
            joined_weight, (first, (1 - core) * width, 0), (size, width, columns)
        )
        theirs = swap(theirs)
        blocks = prepare(joined_weight, theirs, gain if whole else norm_gain, place, first, whole)
        moved.append([exchange(blocks[0], FIRST_GROUPS)] if whole else staged(blocks, first_move))
    outs = []
    found = []
    for first, buffers, whole in zip(firsts, moved, WHOLE):
        if not whole:
            buffers = reorder(buffers)
        else:
            found.append(placed_peaks(peaks(buffers), whole))
        if whole:
            arrived = [exchange(buffers[0], SECOND_GROUPS)]
        else:
            arrived = staged(buffers, second_move)
        own = None if whole else norm_gain
        outs = list(finish(arrived, turns[whole], own, layers, first, outs))
        if not whole:
            found.append(outs.pop()[:, 0].astype(jnp.bfloat16))
    peak = jnp.concatenate(found, axis=0)
    for steps in JOINS:
        others = [lax.ppermute(peak, "ma", [(j, j ^ step) for j in range(16)]) for step in steps]
        for other in others:
            peak = jnp.maximum(peak, other)
    ready, stored = peak[: SIZES[0]], peak[SIZES[0] :].reshape(-1, SLOTS, dim)
    orders = (rotary_order[None, :] == jnp.arange(dim, dtype=jnp.int32)[:, None]).astype(jnp.bfloat16)
    turned = jnp.dot(stored[:, :-1].reshape(-1, dim), orders, preferred_element_type=jnp.float32)
    turned = turned.reshape(-1, SLOTS - 1, dim)
    turned = jnp.concatenate([turned, stored[:, -1:].astype(jnp.float32)], axis=1)
    row_peak = jnp.concatenate([ready.astype(jnp.float32), turned.reshape(-1, SLOTS * dim)], axis=0)
    query, key, value = outs
    return query, key, value, row_peak


JOINS = ((1,), (8,), (2, 4, 6))


def solution(mesh):
    return jax.shard_map(
        shards,
        mesh=mesh,
        in_specs=(P(None, "dev", "ma"), P(None, "ma"), P()),
        out_specs=(
            P(None, "dev", "ma"),
            P(None, "dev", "ma"),
            P(None, "dev", "ma"),
            P(None, "dev"),
        ),
        check_vma=False,
    )
```

```python
import functools

import jax
import jax.numpy as jnp
import numpy as np
from jax import lax
from jax.experimental import pallas as pl
from jax.experimental.pallas import tpu as pltpu
from jax.sharding import PartitionSpec as P


HEADS = 32
KV_HEADS = 8
GROUP = 4
SLOTS = GROUP + 2
HEAD_TOTAL = HEADS + 2 * KV_HEADS
SIZES = (4, 4)
WHOLE = (False, True)
SIDE = 4
STEP = 2
PLACES = 8


def number(a, y, b, x, core):
    return (a * SIDE + y) * 16 + b * 8 + x * 2 + core


def everywhere():
    for n in range(128):
        i, j = divmod(n, 16)
        yield n, i >> 2, i & 3, j >> 3, (j >> 1) & 3, j & 1


def swap(array):
    pairs = [(n, number(a, y, b, x, core ^ 1)) for n, a, y, b, x, core in everywhere()]
    return lax.ppermute(array, ("dev", "ma"), pairs)


def gain_move(gain):
    pairs = [(n, number(b, x, a, y, core)) for n, a, y, b, x, core in everywhere()]
    return lax.ppermute(gain, ("dev", "ma"), pairs)


def first_move(array, r, s):
    pairs = [(n, number(a ^ s, (y + r) % SIDE, b ^ s, x, core)) for n, a, y, b, x, core in everywhere()]
    return lax.ppermute(array, ("dev", "ma"), pairs)


def second_move(array, q, s):
    pairs = [(n, number(a, y, b ^ s, (x + q) % SIDE, core)) for n, a, y, b, x, core in everywhere()]
    return lax.ppermute(array, ("dev", "ma"), pairs)


def position():
    dev = lax.axis_index("dev")
    ma = lax.axis_index("ma")
    return dev >> 2, dev & 3, ma >> 3, (ma >> 1) & 3, ma & 1


def picker(piece):
    columns = piece * HEAD_TOTAL
    pick = np.zeros((columns, columns), np.float32)
    for g in range(KV_HEADS):
        for s in range(SLOTS):
            head = g * GROUP + s if s < GROUP else HEADS + (s - GROUP) * KV_HEADS + g
            for d in range(piece):
                pick[(g * SLOTS + s) * piece + d, d * HEAD_TOTAL + head] = 1.0
    return jnp.asarray(pick, jnp.bfloat16)


def prepare_body(first, place_ref, pick_ref, gain_ref, own_ref, other_ref, *refs):
    out_refs = refs[:-1]
    turned_ref = refs[-1]
    count, width, _ = own_ref.shape
    contract = (((1,), (1,)), ((), ()))
    rows = turned_ref.shape[1] // KV_HEADS
    a = place_ref[1]
    y = place_ref[2]

    def turned(block):
        found = lax.dot_general(pick_ref[...], block, contract, preferred_element_type=jnp.float32)
        return found.reshape(KV_HEADS * SLOTS, -1, width)

    for n in range(count):
        both = jnp.concatenate([turned(own_ref[n]), turned(other_ref[n])], axis=1)
        both = both.reshape(-1, width)
        if len(out_refs) == 1:
            layer = first + pl.program_id(0) * count + n
            both = both * gain_ref[pl.ds(layer, 1), :]
            out_refs[0][:, n] = both.astype(jnp.bfloat16).reshape(KV_HEADS, rows, width)
        else:
            turned_ref[n] = both.astype(jnp.bfloat16)
            for s in range(2):
                for r in range(SIDE):
                    g = (a ^ s) * SIDE + ((y + r) & (SIDE - 1))
                    start = pl.multiple_of(g * rows, 16)
                    out_refs[s * SIDE + r][n] = turned_ref[n, pl.ds(start, rows), :]


def prepare(stored, other, gain, place, first, whole):
    _, features, columns = stored.shape
    layers = other.shape[0]
    width = features // 2
    rows = 2 * columns // KV_HEADS
    step = STEP
    if whole:
        out_specs = [pl.BlockSpec((PLACES, step, rows, width), lambda l, place: (0, l, 0, 0))]
        out_shape = [jax.ShapeDtypeStruct((PLACES, layers, rows, width), jnp.bfloat16)]
    else:
        out_specs = [pl.BlockSpec((step, rows, width), lambda l, place: (l, 0, 0))] * PLACES
        out_shape = [jax.ShapeDtypeStruct((layers, rows, width), jnp.bfloat16)] * PLACES
    return pl.pallas_call(
        functools.partial(prepare_body, first),
        grid_spec=pltpu.PrefetchScalarGridSpec(
            num_scalar_prefetch=1,
            grid=(layers // step,),
            in_specs=[
                pl.BlockSpec((columns, columns), lambda l, place: (0, 0)),
                pl.BlockSpec(gain.shape, lambda l, place: (0, 0)),
                pl.BlockSpec((step, width, columns), lambda l, place: (first // step + l, place[0], 0)),
                pl.BlockSpec((step, width, columns), lambda l, place: (l, 0, 0)),
            ],
            out_specs=out_specs,
            scratch_shapes=[pltpu.VMEM((step, 2 * columns, width), jnp.bfloat16)],
        ),
        out_shape=out_shape,
        name="prepare",
    )(place, picker(columns // HEAD_TOTAL), gain, stored, other)


def reorder_body(*refs):
    in_refs = refs[:PLACES]
    out_refs = refs[PLACES : 2 * PLACES]
    held_ref, in_sems, out_sems = refs[2 * PLACES :]
    a, y, b, x, _ = position()
    flip = a ^ b
    turn = (y - x) & (SIDE - 1)
    for f in range(2):
        for t in range(SIDE):

            @pl.when((flip == f) & (turn == t))
            def _(f=f, t=t):
                for s in range(2):
                    for q in range(SIDE):
                        source = (s ^ f) * SIDE + ((t - q) & (SIDE - 1))
                        k = s * SIDE + q
                        pltpu.make_async_copy(in_refs[source], held_ref.at[k], in_sems.at[k]).start()

    for k in range(PLACES):
        pltpu.make_async_copy(in_refs[k], held_ref.at[k], in_sems.at[k]).wait()
        pltpu.make_async_copy(held_ref.at[k], out_refs[k], out_sems.at[k]).start()
    for k in range(PLACES):
        pltpu.make_async_copy(held_ref.at[k], out_refs[k], out_sems.at[k]).wait()


def reorder(buffers):
    spec = pl.BlockSpec(memory_space=pltpu.HBM)
    shape = buffers[0].shape
    return pl.pallas_call(
        reorder_body,
        in_specs=[spec] * PLACES,
        out_specs=[spec] * PLACES,
        out_shape=[jax.ShapeDtypeStruct(shape, v.dtype) for v in buffers],
        scratch_shapes=[
            pltpu.VMEM((PLACES, *shape), jnp.bfloat16),
            pltpu.SemaphoreType.DMA((PLACES,)),
            pltpu.SemaphoreType.DMA((PLACES,)),
        ],
        name="reorder",
    )(*buffers)


def peak_body(*refs):
    moved_refs, out_ref = refs[:-1], refs[-1]
    _, _, width = moved_refs[0].shape
    for u in range(2):
        size = jnp.abs(moved_refs[u * SIDE][...])
        for v in range(1, SIDE):
            size = jnp.maximum(size, jnp.abs(moved_refs[u * SIDE + v][...]))
        size = size.reshape(-1, width).astype(jnp.float32)
        size = jnp.maximum(size[:, :128], size[:, 128:])
        out_ref[u : u + 1, :] = jnp.max(size.T, axis=0, keepdims=True)


def peaks(moved):
    layers, rows, width = moved[0].shape[-3:]
    if len(moved) == 1:
        held = [
            pl.BlockSpec((None, layers, rows, width), lambda l, k=k: (k, 0, 0, 0)) for k in range(PLACES)
        ]
        moved = moved * PLACES
    else:
        held = [pl.BlockSpec((layers, rows, width), lambda l: (0, 0, 0))] * PLACES
    return pl.pallas_call(
        peak_body,
        grid=(1,),
        in_specs=held,
        out_specs=pl.BlockSpec((2, layers * rows), lambda l: (0, 0)),
        out_shape=jax.ShapeDtypeStruct((2, layers * rows), jnp.float32),
        name="peaks",
    )(*moved)


def placed_peaks(found, whole):
    a, _, b, x, core = position()
    found = found.reshape(2, -1, SLOTS, 2, PLACES)
    found = jnp.where(core == 1, found[:, :, :, ::-1], found)
    u = jnp.arange(2)[:, None]
    upper = u ^ a ^ b if whole else u ^ a
    here = jnp.arange(PLACES)[None, :] == upper * SIDE + x
    spread = jnp.where(here[:, None, None, :, None, None], found[:, :, :, None], 0.0)
    return spread.max(0).reshape(found.shape[1], -1).astype(jnp.bfloat16)


def finish_body(turn_ref, gain_ref, first, *refs):
    moved_refs = refs[:PLACES]
    outs = refs[PLACES:]
    if gain_ref is None:
        query_ref, key_ref, value_ref = outs[-3:]
    else:
        query_ref, key_ref, value_ref, peak_ref = outs[-4:]
    _, rows, _ = moved_refs[0].shape
    piece = rows // SLOTS
    dim = PLACES * piece
    for s in range(SLOTS):
        held = jnp.concatenate([ref[0, s * piece : (s + 1) * piece, :] for ref in moved_refs], axis=0)
        turned = jnp.dot(turn_ref[s // (SLOTS - 1)], held, preferred_element_type=jnp.float32)
        if gain_ref is not None:
            turned = turned * gain_ref[pl.ds(first + pl.program_id(0), 1), :]
        turned = turned.astype(jnp.bfloat16)
        if s < GROUP:
            query_ref[0, s * dim : (s + 1) * dim, :] = turned
        elif s == GROUP:
            key_ref[0] = turned
        else:
            value_ref[0] = turned
        if gain_ref is not None:
            size = jnp.abs(turned.astype(jnp.float32))
            size = jnp.maximum(size[:, :128], size[:, 128:])
            peak_ref[0, :, s * dim : (s + 1) * dim] = jnp.max(size.T, axis=0, keepdims=True)


def plain_body(turn_ref, *refs):
    finish_body(turn_ref, None, 0, *refs)


def scaled_body(first, turn_ref, gain_ref, *refs):
    finish_body(turn_ref, gain_ref, first, *refs)


def finish(moved, turn, gain, whole, first, earlier):
    layers, rows, width = moved[0].shape[-3:]
    dim = turn.shape[1]

    def at(*shape):
        return pl.BlockSpec((1, *shape), lambda l: (first + l, 0, 0))

    shapes = [
        ((GROUP * dim, width), jnp.bfloat16),
        ((dim, width), jnp.bfloat16),
        ((dim, width), jnp.bfloat16),
    ]
    out_specs = [at(*shape) for shape, _ in shapes]
    out_shape = [jax.ShapeDtypeStruct((whole, *shape), kind) for shape, kind in shapes]
    before = [turn]
    in_specs = [pl.BlockSpec((2, dim, dim), lambda l: (0, 0, 0))]
    body = plain_body
    if gain is not None:
        body = functools.partial(scaled_body, first)
        before.append(gain)
        in_specs.append(pl.BlockSpec(gain.shape, lambda l: (0, 0)))
        out_specs.append(pl.BlockSpec((1, 1, SLOTS * dim), lambda l: (l, 0, 0)))
        out_shape.append(jax.ShapeDtypeStruct((layers, 1, SLOTS * dim), jnp.float32))
    if len(moved) == 1:
        held = [
            pl.BlockSpec((None, 1, rows, width), lambda l, k=k: (k, l, 0, 0)) for k in range(PLACES)
        ]
        moved = moved * PLACES
    else:
        held = [pl.BlockSpec((1, rows, width), lambda l: (l, 0, 0))] * PLACES
    shapes = [
        ((GROUP * dim, width), jnp.bfloat16),
        ((dim, width), jnp.bfloat16),
        ((dim, width), jnp.bfloat16),
    ]
    return pl.pallas_call(
        body,
        grid=(layers,),
        in_specs=in_specs + held + [pl.BlockSpec(memory_space=pltpu.HBM)] * len(earlier),
        out_specs=out_specs,
        out_shape=out_shape,
        input_output_aliases={len(before) + PLACES + k: k for k in range(len(earlier))},
        name="finish",
    )(*before, *moved, *earlier)


def turning(rotary_order, whole):
    dim = rotary_order.shape[0]
    piece = dim // PLACES
    a, _, b, x, core = position()
    place = jnp.arange(dim, dtype=jnp.int32)
    u = place // (SIDE * piece)
    v = (place // piece) & (SIDE - 1)
    t = place & (piece - 1)
    high, low = (u ^ a ^ b, v) if whole else (u ^ a, (x - v) & (SIDE - 1))
    holds = (high * SIDE + low) * piece + (t ^ (core * (piece // 2)))
    orders = jnp.stack([rotary_order, place])
    return (orders[:, :, None] == holds[None, None, :]).astype(jnp.bfloat16)


FIRST_GROUPS = [
    [number(a, y, a ^ key, x, core) for a in range(2) for y in range(SIDE)]
    for key in range(2)
    for x in range(SIDE)
    for core in range(2)
]
SECOND_GROUPS = [
    [number(a, y, b, x, core) for b in range(2) for x in range(SIDE)]
    for a in range(2)
    for y in range(SIDE)
    for core in range(2)
]


def exchange(array, groups):
    return lax.all_to_all(array, ("dev", "ma"), 0, 0, tiled=True, axis_index_groups=groups)


STAGE = ((2, 1), (1, 1), (3, 1), (0, 1), (2, 0), (1, 0), (3, 0))

LAST = ((2, 1), (1, 0), (2, 0), (0, 1), (3, 1), (3, 0), (1, 1))


def staged(buffers, move, order):
    out = list(buffers)
    for step, s in order:
        k = s * SIDE + step
        out[k] = move(buffers[k], step, s)
    return out


def shards(joined_weight, norm_gain, rotary_order):
    layers, features, columns = joined_weight.shape
    width = features // 2
    dim = rotary_order.shape[0]
    a, y, _, _, core = position()
    place = jnp.stack([core, a, y]).astype(jnp.int32)
    turns = [turning(rotary_order, False), turning(rotary_order, True)]
    firsts = [sum(SIZES[:k]) for k in range(len(SIZES))]
    gain = gain_move(norm_gain)
    moved = []
    for first, size, whole in zip(firsts, SIZES, WHOLE):
        theirs = lax.dynamic_slice(
            joined_weight, (first, (1 - core) * width, 0), (size, width, columns)
        )
        theirs = swap(theirs)
        blocks = prepare(joined_weight, theirs, gain if whole else norm_gain, place, first, whole)
        moved.append([exchange(blocks[0], FIRST_GROUPS)] if whole else staged(blocks, first_move, STAGE))
    outs = []
    found = []
    for first, buffers, whole in zip(firsts, moved, WHOLE):
        if not whole:
            buffers = reorder(buffers)
        else:
            found.append(placed_peaks(peaks(buffers), whole))
        if whole:
            arrived = [exchange(buffers[0], SECOND_GROUPS)]
        else:
            arrived = staged(buffers, second_move, LAST)
        own = None if whole else norm_gain
        outs = list(finish(arrived, turns[whole], own, layers, first, outs))
        if not whole:
            found.append(outs.pop()[:, 0].astype(jnp.bfloat16))
    peak = jnp.concatenate(found, axis=0)
    for steps in JOINS:
        others = [
            lax.ppermute(peak, "ma", [(j, j ^ step) for j in range(16)]) for step in steps
        ]
        for other in others:
            peak = jnp.maximum(peak, other)
    ready, stored = peak[: SIZES[0]], peak[SIZES[0] :].reshape(-1, SLOTS, dim)
    orders = (rotary_order[None, :] == jnp.arange(dim, dtype=jnp.int32)[:, None]).astype(jnp.bfloat16)
    turned = jnp.dot(stored[:, :-1].reshape(-1, dim), orders, preferred_element_type=jnp.float32)
    turned = turned.reshape(-1, SLOTS - 1, dim)
    turned = jnp.concatenate([turned, stored[:, -1:].astype(jnp.float32)], axis=1)
    row_peak = jnp.concatenate([ready.astype(jnp.float32), turned.reshape(-1, SLOTS * dim)], axis=0)
    query, key, value = outs
    return query, key, value, row_peak


JOINS = ((1,), (8,), (2, 4, 6))


def solution(mesh):
    return jax.shard_map(
        shards,
        mesh=mesh,
        in_specs=(P(None, "dev", "ma"), P(None, "ma"), P()),
        out_specs=(
            P(None, "dev", "ma"),
            P(None, "dev", "ma"),
            P(None, "dev", "ma"),
            P(None, "dev"),
        ),
        check_vma=False,
    )
```

```python
import functools
import itertools

import jax
import jax.numpy as jnp
import numpy as np
from jax import lax
from jax.experimental import pallas as pl
from jax.experimental.pallas import tpu as pltpu
from jax.sharding import PartitionSpec as P


HEADS = 32
KV_HEADS = 8
GROUP = 4
SLOTS = GROUP + 2
HEAD_TOTAL = HEADS + 2 * KV_HEADS
SIZES = (4, 4)
WHOLE = (False, True)
SIDE = 4
STEP = 2
ENDSTEP = 4
PLACES = 8


def number(a, y, b, x, core):
    return (a * SIDE + y) * 16 + b * 8 + x * 2 + core


def everywhere():
    for n in range(128):
        i, j = divmod(n, 16)
        yield n, i >> 2, i & 3, j >> 3, (j >> 1) & 3, j & 1


def swap(array):
    pairs = [(n, number(a, y, b, x, core ^ 1)) for n, a, y, b, x, core in everywhere()]
    return lax.ppermute(array, ("dev", "ma"), pairs)


def gain_move(gain):
    pairs = [(n, number(b, x, a, y, core)) for n, a, y, b, x, core in everywhere()]
    return lax.ppermute(gain, ("dev", "ma"), pairs)


def first_move(array, r, s):
    pairs = [(n, number(a ^ s, (y + r) % SIDE, b ^ s, x, core)) for n, a, y, b, x, core in everywhere()]
    return lax.ppermute(array, ("dev", "ma"), pairs)


def second_move(array, q, s):
    pairs = [(n, number(a, y, b ^ s, (x + q) % SIDE, core)) for n, a, y, b, x, core in everywhere()]
    return lax.ppermute(array, ("dev", "ma"), pairs)


def position():
    dev = lax.axis_index("dev")
    ma = lax.axis_index("ma")
    return dev >> 2, dev & 3, ma >> 3, (ma >> 1) & 3, ma & 1


def picker(piece):
    columns = piece * HEAD_TOTAL
    pick = np.zeros((columns, columns), np.float32)
    for g in range(KV_HEADS):
        for s in range(SLOTS):
            head = g * GROUP + s if s < GROUP else HEADS + (s - GROUP) * KV_HEADS + g
            for d in range(piece):
                pick[(g * SLOTS + s) * piece + d, d * HEAD_TOTAL + head] = 1.0
    return jnp.asarray(pick, jnp.bfloat16)


def prepare_body(first, place_ref, pick_ref, gain_ref, own_ref, other_ref, *refs):
    out_refs = refs[:-1]
    turned_ref = refs[-1]
    count, width, _ = own_ref.shape
    contract = (((1,), (1,)), ((), ()))
    rows = turned_ref.shape[1] // KV_HEADS
    a = place_ref[1]
    y = place_ref[2]

    def turned(block):
        found = lax.dot_general(pick_ref[...], block, contract, preferred_element_type=jnp.float32)
        return found.reshape(KV_HEADS * SLOTS, -1, width)

    for n in range(count):
        both = jnp.concatenate([turned(own_ref[n]), turned(other_ref[n])], axis=1)
        both = both.reshape(-1, width)
        if len(out_refs) == 1:
            layer = first + pl.program_id(0) * count + n
            both = both * gain_ref[pl.ds(layer, 1), :]
            out_refs[0][:, n] = both.astype(jnp.bfloat16).reshape(KV_HEADS, rows, width)
        else:
            turned_ref[n] = both.astype(jnp.bfloat16)
            for s in range(2):
                for r in range(SIDE):
                    g = (a ^ s) * SIDE + ((y + r) & (SIDE - 1))
                    start = pl.multiple_of(g * rows, 16)
                    out_refs[s * SIDE + r][n] = turned_ref[n, pl.ds(start, rows), :]


def prepare(stored, other, gain, place, first, whole):
    _, features, columns = stored.shape
    layers = other.shape[0]
    width = features // 2
    rows = 2 * columns // KV_HEADS
    step = STEP
    if whole:
        out_specs = [pl.BlockSpec((PLACES, step, rows, width), lambda l, place: (0, l, 0, 0))]
        out_shape = [jax.ShapeDtypeStruct((PLACES, layers, rows, width), jnp.bfloat16)]
    else:
        out_specs = [pl.BlockSpec((step, rows, width), lambda l, place: (l, 0, 0))] * PLACES
        out_shape = [jax.ShapeDtypeStruct((layers, rows, width), jnp.bfloat16)] * PLACES
    return pl.pallas_call(
        functools.partial(prepare_body, first),
        grid_spec=pltpu.PrefetchScalarGridSpec(
            num_scalar_prefetch=1,
            grid=(layers // step,),
            in_specs=[
                pl.BlockSpec((columns, columns), lambda l, place: (0, 0)),
                pl.BlockSpec(gain.shape, lambda l, place: (0, 0)),
                pl.BlockSpec((step, width, columns), lambda l, place: (first // step + l, place[0], 0)),
                pl.BlockSpec((step, width, columns), lambda l, place: (l, 0, 0)),
            ],
            out_specs=out_specs,
            scratch_shapes=[pltpu.VMEM((step, 2 * columns, width), jnp.bfloat16)],
        ),
        out_shape=out_shape,
        name="prepare",
    )(place, picker(columns // HEAD_TOTAL), gain, stored, other)


def reorder_body(*refs):
    in_refs = refs[:PLACES]
    out_refs = refs[PLACES : 2 * PLACES]
    held_ref, in_sems, out_sems = refs[2 * PLACES :]
    a, y, b, x, _ = position()
    flip = a ^ b
    turn = (y - x) & (SIDE - 1)
    for f in range(2):
        for t in range(SIDE):

            @pl.when((flip == f) & (turn == t))
            def _(f=f, t=t):
                for s in range(2):
                    for q in range(SIDE):
                        source = (s ^ f) * SIDE + ((t - q) & (SIDE - 1))
                        k = s * SIDE + q
                        pltpu.make_async_copy(in_refs[source], held_ref.at[k], in_sems.at[k]).start()

    for k in range(PLACES):
        pltpu.make_async_copy(in_refs[k], held_ref.at[k], in_sems.at[k]).wait()
        pltpu.make_async_copy(held_ref.at[k], out_refs[k], out_sems.at[k]).start()
    for k in range(PLACES):
        pltpu.make_async_copy(held_ref.at[k], out_refs[k], out_sems.at[k]).wait()


def reorder(buffers):
    spec = pl.BlockSpec(memory_space=pltpu.HBM)
    shape = buffers[0].shape
    return pl.pallas_call(
        reorder_body,
        in_specs=[spec] * PLACES,
        out_specs=[spec] * PLACES,
        out_shape=[jax.ShapeDtypeStruct(shape, v.dtype) for v in buffers],
        scratch_shapes=[
            pltpu.VMEM((PLACES, *shape), jnp.bfloat16),
            pltpu.SemaphoreType.DMA((PLACES,)),
            pltpu.SemaphoreType.DMA((PLACES,)),
        ],
        name="reorder",
    )(*buffers)


def peak_body(*refs):
    moved_refs, out_ref = refs[:-1], refs[-1]
    _, _, width = moved_refs[0].shape
    for u in range(2):
        size = jnp.abs(moved_refs[u * SIDE][...])
        for v in range(1, SIDE):
            size = jnp.maximum(size, jnp.abs(moved_refs[u * SIDE + v][...]))
        size = size.reshape(-1, width).astype(jnp.float32)
        size = jnp.maximum(size[:, :128], size[:, 128:])
        out_ref[u : u + 1, :] = jnp.max(size.T, axis=0, keepdims=True)


def peaks(moved):
    layers, rows, width = moved[0].shape[-3:]
    if len(moved) == 1:
        held = [
            pl.BlockSpec((None, layers, rows, width), lambda l, k=k: (k, 0, 0, 0)) for k in range(PLACES)
        ]
        moved = moved * PLACES
    else:
        held = [pl.BlockSpec((layers, rows, width), lambda l: (0, 0, 0))] * PLACES
    return pl.pallas_call(
        peak_body,
        grid=(1,),
        in_specs=held,
        out_specs=pl.BlockSpec((2, layers * rows), lambda l: (0, 0)),
        out_shape=jax.ShapeDtypeStruct((2, layers * rows), jnp.float32),
        name="peaks",
    )(*moved)


def placed_peaks(found, whole):
    a, _, b, x, core = position()
    found = found.reshape(2, -1, SLOTS, 2, PLACES)
    found = jnp.where(core == 1, found[:, :, :, ::-1], found)
    u = jnp.arange(2)[:, None]
    upper = u ^ a ^ b if whole else u ^ a
    here = jnp.arange(PLACES)[None, :] == upper * SIDE + x
    spread = jnp.where(here[:, None, None, :, None, None], found[:, :, :, None], 0.0)
    return spread.max(0).reshape(found.shape[1], -1).astype(jnp.bfloat16)


def finish_body(turn_ref, gain_ref, first, *refs):
    moved_refs = refs[:PLACES]
    outs = refs[PLACES:]
    if gain_ref is None:
        query_ref, key_ref, value_ref = outs[-3:]
    else:
        query_ref, key_ref, value_ref, peak_ref = outs[-4:]
    count, rows, _ = moved_refs[0].shape
    piece = rows // SLOTS
    dim = PLACES * piece
    for n, s in itertools.product(range(count), range(SLOTS)):
        held = jnp.concatenate([ref[n, s * piece : (s + 1) * piece, :] for ref in moved_refs], axis=0)
        turned = jnp.dot(turn_ref[s // (SLOTS - 1)], held, preferred_element_type=jnp.float32)
        if gain_ref is not None:
            turned = turned * gain_ref[pl.ds(first + pl.program_id(0) * count + n, 1), :]
        turned = turned.astype(jnp.bfloat16)
        if s < GROUP:
            query_ref[n, s * dim : (s + 1) * dim, :] = turned
        elif s == GROUP:
            key_ref[n] = turned
        else:
            value_ref[n] = turned
        if gain_ref is not None:
            size = jnp.abs(turned.astype(jnp.float32))
            size = jnp.maximum(size[:, :128], size[:, 128:])
            peak_ref[n, :, s * dim : (s + 1) * dim] = jnp.max(size.T, axis=0, keepdims=True)


def plain_body(turn_ref, *refs):
    finish_body(turn_ref, None, 0, *refs)


def scaled_body(first, turn_ref, gain_ref, *refs):
    finish_body(turn_ref, gain_ref, first, *refs)


def finish(moved, turn, gain, whole, first, earlier):
    layers, rows, width = moved[0].shape[-3:]
    dim = turn.shape[1]

    def at(*shape):
        return pl.BlockSpec((ENDSTEP, *shape), lambda l: (first // ENDSTEP + l, 0, 0))

    shapes = [
        ((GROUP * dim, width), jnp.bfloat16),
        ((dim, width), jnp.bfloat16),
        ((dim, width), jnp.bfloat16),
    ]
    out_specs = [at(*shape) for shape, _ in shapes]
    out_shape = [jax.ShapeDtypeStruct((whole, *shape), kind) for shape, kind in shapes]
    before = [turn]
    in_specs = [pl.BlockSpec((2, dim, dim), lambda l: (0, 0, 0))]
    body = plain_body
    if gain is not None:
        body = functools.partial(scaled_body, first)
        before.append(gain)
        in_specs.append(pl.BlockSpec(gain.shape, lambda l: (0, 0)))
        out_specs.append(pl.BlockSpec((ENDSTEP, 1, SLOTS * dim), lambda l: (l, 0, 0)))
        out_shape.append(jax.ShapeDtypeStruct((layers, 1, SLOTS * dim), jnp.float32))
    if len(moved) == 1:
        held = [
            pl.BlockSpec((None, ENDSTEP, rows, width), lambda l, k=k: (k, l, 0, 0)) for k in range(PLACES)
        ]
        moved = moved * PLACES
    else:
        held = [pl.BlockSpec((ENDSTEP, rows, width), lambda l: (l, 0, 0))] * PLACES
    shapes = [
        ((GROUP * dim, width), jnp.bfloat16),
        ((dim, width), jnp.bfloat16),
        ((dim, width), jnp.bfloat16),
    ]
    return pl.pallas_call(
        body,
        grid=(layers // ENDSTEP,),
        in_specs=in_specs + held + [pl.BlockSpec(memory_space=pltpu.HBM)] * len(earlier),
        out_specs=out_specs,
        out_shape=out_shape,
        input_output_aliases={len(before) + PLACES + k: k for k in range(len(earlier))},
        name="finish",
    )(*before, *moved, *earlier)


def turning(rotary_order, whole):
    dim = rotary_order.shape[0]
    piece = dim // PLACES
    a, _, b, x, core = position()
    place = jnp.arange(dim, dtype=jnp.int32)
    u = place // (SIDE * piece)
    v = (place // piece) & (SIDE - 1)
    t = place & (piece - 1)
    high, low = (u ^ a ^ b, v) if whole else (u ^ a, (x - v) & (SIDE - 1))
    holds = (high * SIDE + low) * piece + (t ^ (core * (piece // 2)))
    orders = jnp.stack([rotary_order, place])
    return (orders[:, :, None] == holds[None, None, :]).astype(jnp.bfloat16)


FIRST_GROUPS = [
    [number(a, y, a ^ key, x, core) for a in range(2) for y in range(SIDE)]
    for key in range(2)
    for x in range(SIDE)
    for core in range(2)
]
SECOND_GROUPS = [
    [number(a, y, b, x, core) for b in range(2) for x in range(SIDE)]
    for a in range(2)
    for y in range(SIDE)
    for core in range(2)
]


def exchange(array, groups):
    return lax.all_to_all(array, ("dev", "ma"), 0, 0, tiled=True, axis_index_groups=groups)


STAGE = ((2, 1), (1, 1), (3, 1), (0, 1), (2, 0), (1, 0), (3, 0))

LAST = ((3, 1), (1, 0), (2, 1), (2, 0), (0, 1), (3, 0), (1, 1))


def staged(buffers, move, order):
    out = list(buffers)
    for step, s in order:
        k = s * SIDE + step
        out[k] = move(buffers[k], step, s)
    return out


def shards(joined_weight, norm_gain, rotary_order):
    layers, features, columns = joined_weight.shape
    width = features // 2
    dim = rotary_order.shape[0]
    a, y, _, _, core = position()
    place = jnp.stack([core, a, y]).astype(jnp.int32)
    turns = [turning(rotary_order, False), turning(rotary_order, True)]
    firsts = [sum(SIZES[:k]) for k in range(len(SIZES))]
    gain = gain_move(norm_gain)
    moved = []
    for first, size, whole in zip(firsts, SIZES, WHOLE):
        theirs = lax.dynamic_slice(
            joined_weight, (first, (1 - core) * width, 0), (size, width, columns)
        )
        theirs = swap(theirs)
        blocks = prepare(joined_weight, theirs, gain if whole else norm_gain, place, first, whole)
        moved.append([exchange(blocks[0], FIRST_GROUPS)] if whole else staged(blocks, first_move, STAGE))
    outs = []
    found = []
    for first, buffers, whole in zip(firsts, moved, WHOLE):
        if not whole:
            buffers = reorder(buffers)
        else:
            found.append(placed_peaks(peaks(buffers), whole))
        if whole:
            arrived = [exchange(buffers[0], SECOND_GROUPS)]
        else:
            arrived = staged(buffers, second_move, LAST)
        own = None if whole else norm_gain
        outs = list(finish(arrived, turns[whole], own, layers, first, outs))
        if not whole:
            found.append(outs.pop()[:, 0].astype(jnp.bfloat16))
    peak = jnp.concatenate(found, axis=0)
    for steps in JOINS:
        others = [
            lax.ppermute(peak, "ma", [(j, j ^ step) for j in range(16)]) for step in steps
        ]
        for other in others:
            peak = jnp.maximum(peak, other)
    ready, stored = peak[: SIZES[0]], peak[SIZES[0] :].reshape(-1, SLOTS, dim)
    orders = (rotary_order[None, :] == jnp.arange(dim, dtype=jnp.int32)[:, None]).astype(jnp.bfloat16)
    turned = jnp.dot(stored[:, :-1].reshape(-1, dim), orders, preferred_element_type=jnp.float32)
    turned = turned.reshape(-1, SLOTS - 1, dim)
    turned = jnp.concatenate([turned, stored[:, -1:].astype(jnp.float32)], axis=1)
    row_peak = jnp.concatenate([ready.astype(jnp.float32), turned.reshape(-1, SLOTS * dim)], axis=0)
    query, key, value = outs
    return query, key, value, row_peak


JOINS = ((1,), (2, 4, 6), (8,))


def solution(mesh):
    return jax.shard_map(
        shards,
        mesh=mesh,
        in_specs=(P(None, "dev", "ma"), P(None, "ma"), P()),
        out_specs=(
            P(None, "dev", "ma"),
            P(None, "dev", "ma"),
            P(None, "dev", "ma"),
            P(None, "dev"),
        ),
        check_vma=False,
    )
```
